32 devices in a mesh: wide: 8 (over y, x, core), pair: 4 (over z).
Axes of the slice: x: 2, y: 2, z: 4, core: 2. Of those that a mesh axis runs over, the one named last changes fastest.
Arguments:
- rhs: bfloat16 [32768, 512], P(('wide', 'pair')), may hold values from -6 to 6
- coords: bfloat16 [64, 2, 512], P(('wide', 'pair')), may hold values from 0 to 1
- near_index: int32 [64, 3], P(('wide', 'pair')), may hold values from -2 to 2, as said below
- project_basis: bfloat16 [64, 512, 192], P(('wide', 'pair')), may hold values from -0.25 to 0.25
- expand_basis: bfloat16 [64, 512, 192], P(('wide', 'pair')), may hold values from -0.4375 to 0.4375
- transfer: bfloat16 [32, 5, 2, 192, 192], P(('wide', 'pair')), may hold values from -0.3125 to 0.3125
- level_perm: int32 [5, 192], replicated, may hold values from 0 to 191, each once within a row
Outputs:
- applied: bfloat16 [32768, 512], P(('wide', 'pair'))
The draws below stay inside these ranges and needn't reach their ends.
Inputs may be any that keep to these rules, and one draw needn't show every extreme that they name: `near_index`: each row holds 3 different offsets. `level_perm`: each row is a permutation of 0 to 191.
All inputs are finite; a program needn't handle non-finite values.
Results may differ from the reference program's by a relative error of at most 0.0095.
Values may be sent and summed in bfloat16 or wider, within the bound.
A program may use at most 64 MiB of HBM per device.

```python
import math
import jax
import jax.numpy as jnp
from jax import lax

LEAF = 512
LEAVES_DEV = 2
RANK = 192
COLS = 512
NB = 3
LW = 3
LP = 2
DEVICES_ALL = 32
NLEAVES = 64
UNKNOWNS = 32768
N_WIDE = 8
N_PAIR = 4


def draw_near_index(key, part):
    scores = jax.random.randint(key, (NLEAVES, 5), 0, 4096) * 5 + jnp.arange(5, dtype=jnp.int32)[None, :]
    chosen = lax.top_k(scores, NB)[1]
    return (chosen - 2).astype(jnp.int32)


def level_of(rng, dims, shards, least, top_value):
    gain = 1.0
    for position, blocks in shards:
        draws = jax.random.uniform(jax.random.fold_in(jax.random.fold_in(rng, 6), position), (blocks,), jnp.float32, least / len(shards), top_value / len(shards))
        gain = gain * jnp.repeat(jnp.exp(draws), dims[position] // blocks).reshape((-1,) + (1,) * (len(dims) - 1 - position))
    return gain


def bell_draw(stream_key, shape, width, bound, cuts=(), held_as=jnp.bfloat16):
    entries = jax.random.normal(stream_key, shape, jnp.float32) * width
    if len(cuts) > 0:
        entries = level_of(stream_key, shape, cuts, -0.22, 0.18) * entries
    return jnp.clip(entries, min=-bound, max=bound).astype(held_as)


def setup_inputs(seed: int = 0) -> dict:
    key_list = jax.random.split(jax.random.key(seed), 8)
    rhs = bell_draw(key_list[0], (UNKNOWNS, COLS), 1.0, 6.0, ((0, 32),))
    coords = jnp.clip(1.0 * jax.random.uniform(key_list[1], (NLEAVES, 2, LEAF), jnp.float32) ** level_of(key_list[1], (NLEAVES, 2, LEAF), ((0, 32),), -0.2, 0.2), 0.0, 1.0).astype(jnp.bfloat16)
    near_index = draw_near_index(jax.random.fold_in(key_list[7], 71), 0)
    project_basis = bell_draw(key_list[3], (NLEAVES, LEAF, RANK), LEAF ** -0.5, 0.25, ((0, 32),))
    expand_basis = bell_draw(key_list[4], (NLEAVES, LEAF, RANK), RANK ** -0.5, 0.4375, ((0, 32),))
    transfer = bell_draw(key_list[5], (DEVICES_ALL, LW + LP, 2, RANK, RANK), (2 * RANK) ** -0.5, 0.3125, ((0, 32),))
    level_perm = jax.vmap(lambda own: jax.random.permutation(own, RANK))(jax.random.split(key_list[6], (LW + LP))).reshape((LW + LP, RANK)).astype(jnp.int32)
    return dict(rhs=rhs, coords=coords, near_index=near_index, project_basis=project_basis, expand_basis=expand_basis, transfer=transfer, level_perm=level_perm)


softening = 0.0004

def kernel_tile(target, source):
    delta_x = target[0][:, None] - source[0][None, :]
    delta_y = target[1][:, None] - source[1][None, :]
    factor = 0.25 / math.sqrt(target.shape[1])
    return (lax.rsqrt(delta_x * delta_x + delta_y * delta_y + softening) * factor).astype(jnp.bfloat16)

def reference(rhs, coords, near_index, project_basis, expand_basis, transfer, level_perm):
    nleaves = coords.shape[0]
    columns = rhs.shape[1]
    leaves = rhs.reshape(nleaves, LEAF, columns)
    points = coords.astype(jnp.float32)

    def near_leaf(target):
        summed = jnp.zeros((LEAF, columns), jnp.float32)
        for slot in range(NB):
            source = target + near_index[target, slot]
            inside = (source >= 0) & (source < nleaves)
            clipped = jnp.clip(source, 0, nleaves - 1).astype(jnp.int32)
            tile = kernel_tile(points[target], points[clipped])
            product = jnp.dot(tile, leaves[clipped], preferred_element_type=jnp.float32)
            summed = summed + jnp.where(inside, product, jnp.zeros_like(product))
        return summed
    nearby = lax.map(near_leaf, jnp.arange(nleaves, dtype=jnp.int32))
    devices = N_WIDE * N_PAIR
    projected = jnp.einsum('nlr,nlc->nrc', project_basis.astype(jnp.float32), leaves.astype(jnp.float32))
    projected = projected.reshape(devices, LEAVES_DEV, RANK, columns)
    projected = (projected[:, 0] + projected[:, 1]).astype(jnp.bfloat16)
    device_ids = jnp.arange(devices, dtype=jnp.int32)
    wide_id = device_ids // N_PAIR
    pair_id = device_ids % N_PAIR
    for level in range(LW + LP):
        if level < LW:
            partner = jnp.bitwise_xor(wide_id, 1 << level) * N_PAIR + pair_id
        else:
            partner = wide_id * N_PAIR + jnp.bitwise_xor(pair_id, 1 << level - LW)
        partner_rows = projected[partner][:, level_perm[level], :]
        updated = jnp.einsum('drs,dsc->drc', transfer[:, level, 0].astype(jnp.float32), projected.astype(jnp.float32))
        updated = updated + jnp.einsum('drs,dsc->drc', transfer[:, level, 1].astype(jnp.float32), partner_rows.astype(jnp.float32))
        projected = updated.astype(jnp.bfloat16)
    expand_rows = expand_basis.reshape(devices, LEAVES_DEV * LEAF, RANK).astype(jnp.float32)
    distant = jnp.einsum('dlr,drc->dlc', expand_rows, projected.astype(jnp.float32))
    summed = nearby.reshape(-1, columns) + distant.reshape(-1, columns)
    return summed.astype(jnp.bfloat16)
```

```python
import functools
import math

import jax
import jax.numpy as jnp
from jax import lax
from jax.experimental import pallas as pl
from jax.experimental.pallas import tpu as pltpu
from jax.sharding import PartitionSpec as P

NB = 3
LW = 3
SOFTENING = 0.0004
MESH = pl.DeviceIdType.MESH
PIECES = 4
FIRST = 4
SECOND = 2


def kernel(
    sizes,
    near_ref,
    rhs_ref,
    coords_ref,
    project_ref,
    expand_ref,
    transfer_ref,
    perm_ref,
    out_ref,
    below_ref,
    above_ref,
    below_raw,
    above_raw,
    points,
    targets,
    total,
    state,
    partner_state,
    partner_transfer,
    up_send,
    down_send,
    below_recv,
    above_recv,
    point_send,
    point_recv,
    level_send,
    level_recv,
):
    wide_count, pair_count = sizes
    leaves, _, leaf_rows = coords_ref.shape
    levels, rank = perm_ref.shape
    piece = leaf_rows // PIECES
    wide, pair = lax.axis_index("wide"), lax.axis_index("pair")
    count = wide_count * pair_count
    me = wide * pair_count + pair
    not_first = me > 0
    not_last = me < count - 1

    def place(device):
        return (lax.div(device, pair_count), lax.rem(device, pair_count))

    up = place(lax.rem(me + 1, count))
    down = place(lax.rem(me + count - 1, count))

    def partner(level):
        if level < LW:
            bit = 1 << level
            digit = lax.rem(lax.div(wide, bit), 2)
            return (wide + bit - 2 * bit * digit, pair)
        bit = 1 << (level - LW)
        digit = lax.rem(lax.div(pair, bit), 2)
        return (wide, pair + bit - 2 * bit * digit)

    barrier = pltpu.get_barrier_semaphore()
    peers = [up, down] + [partner(level) for level in range(levels)]
    for peer in peers:
        pl.semaphore_signal(barrier, inc=1, device_id=peer, device_id_type=MESH)

    @pl.when(jnp.logical_not(not_first))
    def _():
        below_ref[...] = jnp.zeros_like(below_ref)
        below_raw[...] = jnp.zeros_like(below_raw)

    @pl.when(jnp.logical_not(not_last))
    def _():
        above_ref[...] = jnp.zeros_like(above_ref)
        above_raw[...] = jnp.zeros_like(above_raw)

    pl.semaphore_wait(barrier, len(peers))

    def rows_up(c):
        leaf = leaves - 1 - lax.div(c, PIECES)
        return pl.ds(pl.multiple_of(leaf * leaf_rows + lax.rem(c, PIECES) * piece, piece), piece)

    def rows_down(c):
        return pl.ds(pl.multiple_of(c * piece, piece), piece)

    def copy_up(c):
        return pltpu.make_async_remote_copy(
            src_ref=rhs_ref.at[rows_up(c)],
            dst_ref=below_ref.at[rows_up(c)],
            send_sem=up_send.at[c],
            recv_sem=below_recv.at[c],
            device_id=up,
            device_id_type=MESH,
        )

    def copy_down(c):
        return pltpu.make_async_remote_copy(
            src_ref=rhs_ref.at[rows_down(c)],
            dst_ref=above_ref.at[rows_down(c)],
            send_sem=down_send.at[c],
            recv_sem=above_recv.at[c],
            device_id=down,
            device_id_type=MESH,
        )

    def point_copy(way, target, destination):
        return pltpu.make_async_remote_copy(
            src_ref=coords_ref,
            dst_ref=destination,
            send_sem=point_send.at[way],
            recv_sem=point_recv.at[way],
            device_id=target,
            device_id_type=MESH,
        )

    points_up = point_copy(0, up, below_raw)
    points_down = point_copy(1, down, above_raw)

    def send_halo(low, high):
        @pl.loop(low, high)
        def _(c):
            @pl.when(not_first)
            def _():
                copy_down(c).start()

            @pl.when(not_last)
            def _():
                copy_up(c).start()

    def level_copy(level):
        return pltpu.make_async_remote_copy(
            src_ref=state.at[level],
            dst_ref=partner_state.at[level],
            send_sem=level_send.at[level],
            recv_sem=level_recv.at[level],
            device_id=partner(level),
            device_id_type=MESH,
        )

    @pl.when(not_last)
    def _():
        points_up.start()

    @pl.when(not_first)
    def _():
        points_down.start()

    send_halo(0, FIRST)

    def dot(a, b, contract=(1, 0)):
        return lax.dot_general(
            a, b, (((contract[0],), (contract[1],)), ((), ())), preferred_element_type=jnp.float32
        )

    projected = sum(
        dot(project_ref[leaf], rhs_ref[leaf * leaf_rows : (leaf + 1) * leaf_rows])
        for leaf in range(leaves)
    )
    state[0] = projected.astype(jnp.bfloat16)
    level_copy(0).start()

    rank_rows = lax.broadcasted_iota(jnp.int32, (rank, rank), 0)
    for level in range(levels):
        chosen = jnp.where(rank_rows == perm_ref[level : level + 1, :], 1.0, 0.0)
        partner_transfer[level] = dot(
            transfer_ref[0, level, 1], chosen.astype(jnp.bfloat16), (1, 1)
        ).astype(jnp.bfloat16)

    for leaf in range(leaves):
        own = coords_ref[leaf].astype(jnp.float32)
        points[leaf + leaves] = own
        for axis in range(2):
            targets[leaf, axis] = jnp.broadcast_to(own[axis : axis + 1, :], (piece, leaf_rows)).T
    total[...] = jnp.zeros_like(total)

    factor = 0.25 / math.sqrt(leaf_rows)

    def scale(target, offset):
        inside = (me * leaves + target + offset >= 0) & (me * leaves + target + offset < count * leaves)
        found = near_ref[target, 0] == offset
        for slot in range(1, NB):
            found = found | (near_ref[target, slot] == offset)
        return jnp.where(found & inside, jnp.float32(factor), jnp.float32(0.0))

    def tile(target, source, c):
        columns = pl.ds(pl.multiple_of(c * piece, piece), piece)
        x = points[source + leaves, 0:1, columns]
        y = points[source + leaves, 1:2, columns]
        dx = targets[target, 0] - x
        dy = targets[target, 1] - y
        value = lax.rsqrt(dx * dx + dy * dy + SOFTENING) * scale(target, source - target)
        return value.astype(jnp.bfloat16)

    def rows_of(source, c):
        leaf = source % leaves
        rows = pl.ds(pl.multiple_of(leaf * leaf_rows + c * piece, piece), piece)
        ref = rhs_ref if 0 <= source < leaves else (below_ref if source < 0 else above_ref)
        return ref[rows, :]

    def near(target, sources, c):
        tiles = jnp.concatenate([tile(target, source, c) for source in sources], axis=1)
        block = jnp.concatenate([rows_of(source, c) for source in sources], axis=0)
        total[target] += dot(tiles, block)

    def near_own(low, high):
        @pl.loop(low, high)
        def _(c):
            for target in range(leaves):
                near(target, list(range(leaves)), c)

    done = 0
    for level in range(levels):
        own_part = dot(transfer_ref[0, level, 0], state[level])
        if done < PIECES:
            near_own(done, done + 1)
            done += 1
        level_copy(level).wait_recv()
        state[level + 1] = (
            own_part + dot(partner_transfer[level], partner_state[level])
        ).astype(jnp.bfloat16)
        if level + 1 < levels:
            level_copy(level + 1).start()
        if level + 1 == LW:
            send_halo(FIRST, FIRST + SECOND)
        if level + 1 == LW + 1:
            send_halo(FIRST + SECOND, leaves * PIECES)
    for leaf in range(leaves):
        total[leaf] += dot(expand_ref[leaf], state[levels], (0, 0))

    @pl.when(not_first)
    def _():
        points_up.wait_recv()

    @pl.when(not_last)
    def _():
        points_down.wait_recv()

    for leaf in range(leaves):
        points[leaf] = below_raw[leaf].astype(jnp.float32)
        points[leaf + 2 * leaves] = above_raw[leaf].astype(jnp.float32)

    for phase in range(leaves):
        low, high = -1 - phase, leaves + phase

        @pl.loop(0, PIECES)
        def _(c):
            at = phase * PIECES + c

            @pl.when(not_first)
            def _():
                copy_up(at).wait_recv()

            @pl.when(not_last)
            def _():
                copy_down(at).wait_recv()

            for target in range(leaves):
                sources = [s for s in (low, high) if abs(s - target) <= leaves]
                near(target, sources, c)

    out_ref[...] = total[...].astype(out_ref.dtype)

    for level in range(levels):
        level_copy(level).wait_send()

    @pl.when(not_last)
    def _():
        points_up.wait_send()

        @pl.loop(0, leaves * PIECES)
        def _(c):
            copy_up(c).wait_send()

    @pl.when(not_first)
    def _():
        points_down.wait_send()

        @pl.loop(0, leaves * PIECES)
        def _(c):
            copy_down(c).wait_send()


def on_device(sizes, rhs, coords, near_index, project_basis, expand_basis, transfer, level_perm):
    leaves, _, leaf_rows = coords.shape
    rows, columns = rhs.shape
    levels, rank = level_perm.shape
    pieces = leaves * PIECES
    dma = pltpu.SemaphoreType.DMA
    vmem = pl.BlockSpec(memory_space=pltpu.VMEM)
    smem = pl.BlockSpec(memory_space=pltpu.SMEM)
    out = pl.pallas_call(
        functools.partial(kernel, sizes),
        out_shape=jax.ShapeDtypeStruct((leaves, leaf_rows, columns), jnp.bfloat16),
        in_specs=[smem] + [vmem] * 6,
        out_specs=vmem,
        scratch_shapes=[
            pltpu.VMEM((rows, columns), jnp.bfloat16),
            pltpu.VMEM((rows, columns), jnp.bfloat16),
            pltpu.VMEM(coords.shape, coords.dtype),
            pltpu.VMEM(coords.shape, coords.dtype),
            pltpu.VMEM((3 * leaves, 2, leaf_rows), jnp.float32),
            pltpu.VMEM((leaves, 2, leaf_rows, leaf_rows // PIECES), jnp.float32),
            pltpu.VMEM((leaves, leaf_rows, columns), jnp.float32),
            pltpu.VMEM((levels + 1, rank, columns), jnp.bfloat16),
            pltpu.VMEM((levels, rank, columns), jnp.bfloat16),
            pltpu.VMEM((levels, rank, rank), jnp.bfloat16),
            dma((pieces,)),
            dma((pieces,)),
            dma((pieces,)),
            dma((pieces,)),
            dma((2,)),
            dma((2,)),
            dma((levels,)),
            dma((levels,)),
        ],
        compiler_params=pltpu.CompilerParams(
            collective_id=0, has_side_effects=True, vmem_limit_bytes=48 * 1024 * 1024
        ),
        name="operator",
    )(
        near_index,
        rhs,
        coords,
        project_basis.swapaxes(1, 2),
        expand_basis.swapaxes(1, 2),
        transfer,
        level_perm,
    )
    return out.reshape(rows, columns)


def solution(mesh):
    sizes = (mesh.shape["wide"], mesh.shape["pair"])
    return jax.shard_map(
        functools.partial(on_device, sizes),
        mesh=mesh,
        in_specs=(
            P(("wide", "pair"), None),
            P(("wide", "pair"), None, None),
            P(("wide", "pair"), None),
            P(("wide", "pair"), None, None),
            P(("wide", "pair"), None, None),
            P(("wide", "pair"), None, None, None, None),
            P(),
        ),
        out_specs=P(("wide", "pair"), None),
        check_vma=False,
    )
```

```python
import functools
import math

import jax
import jax.numpy as jnp
from jax import lax
from jax.experimental import pallas as pl
from jax.experimental.pallas import tpu as pltpu
from jax.sharding import PartitionSpec as P

NB = 3
LW = 3
SOFTENING = 0.0004
MESH = pl.DeviceIdType.MESH
PIECES = 4
VMEM_GRANT = 65000000
FIRST = 3
SECOND = 2


def kernel(
    sizes,
    near_hbm,
    rhs_hbm,
    coords_hbm,
    project_hbm,
    expand_hbm,
    transfer_hbm,
    perm_hbm,
    out_ref,
    near_ref,
    rhs_ref,
    coords_ref,
    project_ref,
    expand_ref,
    transfer_ref,
    perm_ref,
    load_sem,
    below_ref,
    above_ref,
    below_raw,
    above_raw,
    points,
    targets,
    total,
    state,
    partner_state,
    partner_transfer,
    up_send,
    down_send,
    below_recv,
    above_recv,
    point_send,
    point_recv,
    level_send,
    level_recv,
):
    wide_count, pair_count = sizes
    leaves, _, leaf_rows = coords_ref.shape
    levels, rank = perm_ref.shape
    piece = leaf_rows // PIECES
    wide, pair = lax.axis_index("wide"), lax.axis_index("pair")
    count = wide_count * pair_count
    me = wide * pair_count + pair
    not_first = me > 0
    not_last = me < count - 1

    def place(device):
        return (lax.div(device, pair_count), lax.rem(device, pair_count))

    up = place(lax.rem(me + 1, count))
    down = place(lax.rem(me + count - 1, count))

    def partner(level):
        if level < LW:
            bit = 1 << level
            digit = lax.rem(lax.div(wide, bit), 2)
            return (wide + bit - 2 * bit * digit, pair)
        bit = 1 << (level - LW)
        digit = lax.rem(lax.div(pair, bit), 2)
        return (wide, pair + bit - 2 * bit * digit)

    loads = [
        pltpu.make_async_copy(source, destination, load_sem.at[i])
        for i, (source, destination) in enumerate(
            (
                (project_hbm, project_ref),
                (rhs_hbm, rhs_ref),
                (perm_hbm, perm_ref),
                (transfer_hbm, transfer_ref),
                (coords_hbm, coords_ref),
                (near_hbm, near_ref),
                (expand_hbm, expand_ref),
            )
        )
    ]
    barrier = pltpu.get_barrier_semaphore()
    peers = [up, down] + [partner(level) for level in range(levels)]
    for peer in peers:
        pl.semaphore_signal(barrier, inc=1, device_id=peer, device_id_type=MESH)
    for load in loads:
        load.start()

    @pl.when(jnp.logical_not(not_first))
    def _():
        below_ref[...] = jnp.zeros_like(below_ref)
        below_raw[...] = jnp.zeros_like(below_raw)

    @pl.when(jnp.logical_not(not_last))
    def _():
        above_ref[...] = jnp.zeros_like(above_ref)
        above_raw[...] = jnp.zeros_like(above_raw)

    pl.semaphore_wait(barrier, len(peers))

    def rows_up(c):
        leaf = leaves - 1 - lax.div(c, PIECES)
        return pl.ds(pl.multiple_of(leaf * leaf_rows + lax.rem(c, PIECES) * piece, piece), piece)

    def rows_down(c):
        return pl.ds(pl.multiple_of(c * piece, piece), piece)

    def copy_up(c):
        return pltpu.make_async_remote_copy(
            src_ref=rhs_hbm.at[rows_up(c)],
            dst_ref=below_ref.at[rows_up(c)],
            send_sem=up_send.at[c],
            recv_sem=below_recv.at[c],
            device_id=up,
            device_id_type=MESH,
        )

    def copy_down(c):
        return pltpu.make_async_remote_copy(
            src_ref=rhs_hbm.at[rows_down(c)],
            dst_ref=above_ref.at[rows_down(c)],
            send_sem=down_send.at[c],
            recv_sem=above_recv.at[c],
            device_id=down,
            device_id_type=MESH,
        )

    def point_copy(way, target, destination):
        return pltpu.make_async_remote_copy(
            src_ref=coords_hbm,
            dst_ref=destination,
            send_sem=point_send.at[way],
            recv_sem=point_recv.at[way],
            device_id=target,
            device_id_type=MESH,
        )

    points_up = point_copy(0, up, below_raw)
    points_down = point_copy(1, down, above_raw)

    def send_halo(low, high):
        @pl.loop(low, high)
        def _(c):
            @pl.when(not_first)
            def _():
                copy_down(c).start()

            @pl.when(not_last)
            def _():
                copy_up(c).start()

    def level_copy(level):
        return pltpu.make_async_remote_copy(
            src_ref=state.at[level],
            dst_ref=partner_state.at[level],
            send_sem=level_send.at[level],
            recv_sem=level_recv.at[level],
            device_id=partner(level),
            device_id_type=MESH,
        )

    @pl.when(not_last)
    def _():
        points_up.start()

    @pl.when(not_first)
    def _():
        points_down.start()

    send_halo(0, FIRST)

    def dot(a, b, contract=(1, 0)):
        return lax.dot_general(
            a, b, (((contract[0],), (contract[1],)), ((), ())), preferred_element_type=jnp.float32
        )

    loads[0].wait()
    loads[1].wait()
    projected = sum(
        dot(project_ref[leaf], rhs_ref[leaf * leaf_rows : (leaf + 1) * leaf_rows])
        for leaf in range(leaves)
    )
    state[0] = projected.astype(jnp.bfloat16)
    level_copy(0).start()

    loads[2].wait()
    loads[3].wait()
    rank_rows = lax.broadcasted_iota(jnp.int32, (rank, rank), 0)
    for level in range(levels):
        chosen = jnp.where(rank_rows == perm_ref[level : level + 1, :], 1.0, 0.0)
        partner_transfer[level] = dot(
            transfer_ref[0, level, 1], chosen.astype(jnp.bfloat16), (1, 1)
        ).astype(jnp.bfloat16)

    loads[4].wait()
    loads[5].wait()
    for leaf in range(leaves):
        own = coords_ref[leaf].astype(jnp.float32)
        points[leaf + leaves] = own
        for axis in range(2):
            targets[leaf, axis] = jnp.broadcast_to(own[axis : axis + 1, :], (piece, leaf_rows)).T
    total[...] = jnp.zeros_like(total)

    factor = 0.25 / math.sqrt(leaf_rows)

    def scale(target, offset):
        inside = (me * leaves + target + offset >= 0) & (me * leaves + target + offset < count * leaves)
        found = near_ref[target, 0] == offset
        for slot in range(1, NB):
            found = found | (near_ref[target, slot] == offset)
        return jnp.where(found & inside, jnp.float32(factor), jnp.float32(0.0))

    def tile(target, source, c):
        columns = pl.ds(pl.multiple_of(c * piece, piece), piece)
        x = points[source + leaves, 0:1, columns]
        y = points[source + leaves, 1:2, columns]
        dx = targets[target, 0] - x
        dy = targets[target, 1] - y
        value = lax.rsqrt(dx * dx + dy * dy + SOFTENING) * scale(target, source - target)
        return value.astype(jnp.bfloat16)

    def rows_of(source, c):
        leaf = source % leaves
        rows = pl.ds(pl.multiple_of(leaf * leaf_rows + c * piece, piece), piece)
        ref = rhs_ref if 0 <= source < leaves else (below_ref if source < 0 else above_ref)
        return ref[rows, :]

    def near(target, sources, c):
        tiles = jnp.concatenate([tile(target, source, c) for source in sources], axis=1)
        block = jnp.concatenate([rows_of(source, c) for source in sources], axis=0)
        total[target] += dot(tiles, block)

    def near_own(low, high):
        @pl.loop(low, high)
        def _(c):
            for target in range(leaves):
                near(target, list(range(leaves)), c)

    done = 0
    for level in range(levels):
        own_part = dot(transfer_ref[0, level, 0], state[level])
        if done < PIECES:
            near_own(done, done + 1)
            done += 1
        level_copy(level).wait_recv()
        state[level + 1] = (
            own_part + dot(partner_transfer[level], partner_state[level])
        ).astype(jnp.bfloat16)
        if level + 1 < levels:
            level_copy(level + 1).start()
        if level + 1 == LW:
            send_halo(FIRST, FIRST + SECOND)
        if level + 1 == LW + 1:
            send_halo(FIRST + SECOND, leaves * PIECES)
    loads[6].wait()
    for leaf in range(leaves):
        total[leaf] += dot(expand_ref[leaf], state[levels], (0, 0))

    @pl.when(not_first)
    def _():
        points_up.wait_recv()

    @pl.when(not_last)
    def _():
        points_down.wait_recv()

    for leaf in range(leaves):
        points[leaf] = below_raw[leaf].astype(jnp.float32)
        points[leaf + 2 * leaves] = above_raw[leaf].astype(jnp.float32)

    for phase in range(leaves):
        low, high = -1 - phase, leaves + phase

        @pl.loop(0, PIECES)
        def _(c):
            at = phase * PIECES + c

            @pl.when(not_first)
            def _():
                copy_up(at).wait_recv()

            @pl.when(not_last)
            def _():
                copy_down(at).wait_recv()

            for target in range(leaves):
                sources = [s for s in (low, high) if abs(s - target) <= leaves]
                near(target, sources, c)

    out_ref[...] = total[...].astype(out_ref.dtype)

    for level in range(levels):
        level_copy(level).wait_send()

    @pl.when(not_last)
    def _():
        points_up.wait_send()

        @pl.loop(0, leaves * PIECES)
        def _(c):
            copy_up(c).wait_send()

    @pl.when(not_first)
    def _():
        points_down.wait_send()

        @pl.loop(0, leaves * PIECES)
        def _(c):
            copy_down(c).wait_send()


def on_device(sizes, rhs, coords, near_index, project_basis, expand_basis, transfer, level_perm):
    leaves, _, leaf_rows = coords.shape
    rows, columns = rhs.shape
    levels, rank = level_perm.shape
    pieces = leaves * PIECES
    dma = pltpu.SemaphoreType.DMA
    vmem = pl.BlockSpec(memory_space=pltpu.VMEM)
    hbm = pl.BlockSpec(memory_space=pltpu.HBM)
    operands = (
        near_index,
        rhs,
        coords,
        project_basis.swapaxes(1, 2),
        expand_basis.swapaxes(1, 2),
        transfer,
        level_perm,
    )
    out = pl.pallas_call(
        functools.partial(kernel, sizes),
        out_shape=pltpu.VMEM((leaves, leaf_rows, columns), jnp.bfloat16),
        in_specs=[hbm] * len(operands),
        out_specs=vmem,
        scratch_shapes=[pltpu.SMEM(near_index.shape, near_index.dtype)]
        + [pltpu.VMEM(operand.shape, operand.dtype) for operand in operands[1:]]
        + [
            dma((len(operands),)),
            pltpu.VMEM((rows, columns), jnp.bfloat16),
            pltpu.VMEM((rows, columns), jnp.bfloat16),
            pltpu.VMEM(coords.shape, coords.dtype),
            pltpu.VMEM(coords.shape, coords.dtype),
            pltpu.VMEM((3 * leaves, 2, leaf_rows), jnp.float32),
            pltpu.VMEM((leaves, 2, leaf_rows, leaf_rows // PIECES), jnp.float32),
            pltpu.VMEM((leaves, leaf_rows, columns), jnp.float32),
            pltpu.VMEM((levels + 1, rank, columns), jnp.bfloat16),
            pltpu.VMEM((levels, rank, columns), jnp.bfloat16),
            pltpu.VMEM((levels, rank, rank), jnp.bfloat16),
            dma((pieces,)),
            dma((pieces,)),
            dma((pieces,)),
            dma((pieces,)),
            dma((2,)),
            dma((2,)),
            dma((levels,)),
            dma((levels,)),
        ],
        compiler_params=pltpu.CompilerParams(
            collective_id=0, has_side_effects=True, vmem_limit_bytes=VMEM_GRANT
        ),
        name="operator",
    )(*operands)
    return out.reshape(rows, columns)


def solution(mesh):
    sizes = (mesh.shape["wide"], mesh.shape["pair"])
    return jax.shard_map(
        functools.partial(on_device, sizes),
        mesh=mesh,
        in_specs=(
            P(("wide", "pair"), None),
            P(("wide", "pair"), None, None),
            P(("wide", "pair"), None),
            P(("wide", "pair"), None, None),
            P(("wide", "pair"), None, None),
            P(("wide", "pair"), None, None, None, None),
            P(),
        ),
        out_specs=P(("wide", "pair"), None),
        check_vma=False,
    )
```

```python
import functools
import math

import jax
import jax.numpy as jnp
from jax import lax
from jax.experimental import pallas as pl
from jax.experimental.pallas import tpu as pltpu
from jax.sharding import PartitionSpec as P

NB = 3
LW = 3
SOFTENING = 0.0004
MESH = pl.DeviceIdType.MESH
PIECES = 4
VMEM_GRANT = 65000000
FIRST = 4
MOVED = 2
SECOND = 2


def kernel(
    sizes,
    near_hbm,
    rhs_hbm,
    coords_hbm,
    project_hbm,
    expand_hbm,
    transfer_hbm,
    perm_hbm,
    out_ref,
    near_ref,
    rhs_ref,
    coords_ref,
    project_ref,
    expand_ref,
    transfer_ref,
    perm_ref,
    load_sem,
    below_ref,
    above_ref,
    below_raw,
    above_raw,
    points,
    targets,
    total,
    state,
    partner_state,
    partner_transfer,
    up_send,
    down_send,
    below_recv,
    above_recv,
    point_send,
    point_recv,
    level_send,
    level_recv,
    relay_ref,
    relay_send,
    relay_recv,
):
    wide_count, pair_count = sizes
    leaves, _, leaf_rows = coords_ref.shape
    levels, rank = perm_ref.shape
    piece = leaf_rows // PIECES
    wide, pair = lax.axis_index("wide"), lax.axis_index("pair")
    count = wide_count * pair_count
    me = wide * pair_count + pair
    not_first = me > 0
    not_last = me < count - 1

    def place(device):
        return (lax.div(device, pair_count), lax.rem(device, pair_count))

    up = place(lax.rem(me + 1, count))
    down = place(lax.rem(me + count - 1, count))

    def partner(level):
        if level < LW:
            bit = 1 << level
            digit = lax.rem(lax.div(wide, bit), 2)
            return (wide + bit - 2 * bit * digit, pair)
        bit = 1 << (level - LW)
        digit = lax.rem(lax.div(pair, bit), 2)
        return (wide, pair + bit - 2 * bit * digit)

    loads = [
        pltpu.make_async_copy(source, destination, load_sem.at[i])
        for i, (source, destination) in enumerate(
            (
                (project_hbm, project_ref),
                (rhs_hbm, rhs_ref),
                (perm_hbm, perm_ref),
                (transfer_hbm, transfer_ref),
                (coords_hbm, coords_ref),
                (near_hbm, near_ref),
                (expand_hbm, expand_ref),
            )
        )
    ]
    barrier = pltpu.get_barrier_semaphore()
    peers = [up, down] + [partner(level) for level in range(levels)]
    for peer in peers:
        pl.semaphore_signal(barrier, inc=1, device_id=peer, device_id_type=MESH)
    end = pair_count - 1
    slots = wide_count // 2 - 1
    far_up = (lax.rem(wide, 2) == 1) & (wide < wide_count - 1) & (pair == end)
    far_down = (lax.rem(wide, 2) == 0) & (wide > 0) & (pair == 0)
    relay_up = (wide >= wide_count - MOVED) & (pair == end)
    relay_down = (wide < MOVED) & (pair == 0)

    def greet(peer):
        pl.semaphore_signal(barrier, inc=1, device_id=peer, device_id_type=MESH)

    @pl.when(far_up | far_down)
    def _():
        for m in range(MOVED):
            greet((wide_count - MOVED + m, end))
            greet((m, 0))

    @pl.when(relay_up | relay_down)
    def _():
        for slot in range(slots):
            greet((2 * slot + 1, end))
            greet((2 * slot + 2, 0))

    for load in loads:
        load.start()

    @pl.when(jnp.logical_not(not_first))
    def _():
        below_ref[...] = jnp.zeros_like(below_ref)
        below_raw[...] = jnp.zeros_like(below_raw)

    @pl.when(jnp.logical_not(not_last))
    def _():
        above_ref[...] = jnp.zeros_like(above_ref)
        above_raw[...] = jnp.zeros_like(above_raw)

    extra = jnp.where(far_up | far_down, 2 * MOVED, 0)
    extra = extra + jnp.where(relay_up | relay_down, 2 * slots, 0)
    pl.semaphore_wait(barrier, len(peers) + extra)

    def rows_up(c):
        leaf = leaves - 1 - lax.div(c, PIECES)
        return pl.ds(pl.multiple_of(leaf * leaf_rows + lax.rem(c, PIECES) * piece, piece), piece)

    def rows_down(c):
        return pl.ds(pl.multiple_of(c * piece, piece), piece)

    def copy_up(c):
        return pltpu.make_async_remote_copy(
            src_ref=rhs_hbm.at[rows_up(c)],
            dst_ref=below_ref.at[rows_up(c)],
            send_sem=up_send.at[c],
            recv_sem=below_recv.at[c],
            device_id=up,
            device_id_type=MESH,
        )

    def copy_down(c):
        return pltpu.make_async_remote_copy(
            src_ref=rhs_hbm.at[rows_down(c)],
            dst_ref=above_ref.at[rows_down(c)],
            send_sem=down_send.at[c],
            recv_sem=above_recv.at[c],
            device_id=down,
            device_id_type=MESH,
        )

    def point_copy(way, target, destination):
        return pltpu.make_async_remote_copy(
            src_ref=coords_hbm,
            dst_ref=destination,
            send_sem=point_send.at[way],
            recv_sem=point_recv.at[way],
            device_id=target,
            device_id_type=MESH,
        )

    points_up = point_copy(0, up, below_raw)
    points_down = point_copy(1, down, above_raw)

    def to_relay(rows, send_sem, slot, relay):
        return pltpu.make_async_remote_copy(
            src_ref=rhs_hbm.at[rows],
            dst_ref=relay_ref.at[slot],
            send_sem=send_sem,
            recv_sem=relay_recv.at[slot],
            device_id=relay,
            device_id_type=MESH,
        )

    def onward_up(slot):
        c = wide - (wide_count - MOVED)
        return pltpu.make_async_remote_copy(
            src_ref=relay_ref.at[slot],
            dst_ref=below_ref.at[rows_up(c)],
            send_sem=relay_send.at[slot],
            recv_sem=below_recv.at[c],
            device_id=(2 * slot + 2, 0),
            device_id_type=MESH,
        )

    def onward_down(slot):
        return pltpu.make_async_remote_copy(
            src_ref=relay_ref.at[slot],
            dst_ref=above_ref.at[rows_down(wide)],
            send_sem=relay_send.at[slot],
            recv_sem=above_recv.at[wide],
            device_id=(2 * slot + 1, end),
            device_id_type=MESH,
        )

    def send_halo(low, high):
        @pl.loop(low, high)
        def _(c):
            by_relay_down = far_down & (c < MOVED)
            by_relay_up = far_up & (c < MOVED)

            @pl.when(by_relay_down)
            def _():
                to_relay(rows_down(c), down_send.at[c], lax.div(wide, 2) - 1, (c, 0)).start()

            @pl.when(not_first & jnp.logical_not(by_relay_down))
            def _():
                copy_down(c).start()

            @pl.when(by_relay_up)
            def _():
                to_relay(
                    rows_up(c), up_send.at[c], lax.div(wide, 2), (wide_count - MOVED + c, end)
                ).start()

            @pl.when(not_last & jnp.logical_not(by_relay_up))
            def _():
                copy_up(c).start()

    def level_copy(level):
        return pltpu.make_async_remote_copy(
            src_ref=state.at[level],
            dst_ref=partner_state.at[level],
            send_sem=level_send.at[level],
            recv_sem=level_recv.at[level],
            device_id=partner(level),
            device_id_type=MESH,
        )

    @pl.when(not_last)
    def _():
        points_up.start()

    @pl.when(not_first)
    def _():
        points_down.start()

    send_halo(0, FIRST)

    def dot(a, b, contract=(1, 0)):
        return lax.dot_general(
            a, b, (((contract[0],), (contract[1],)), ((), ())), preferred_element_type=jnp.float32
        )

    loads[0].wait()
    loads[1].wait()
    projected = sum(
        dot(project_ref[leaf], rhs_ref[leaf * leaf_rows : (leaf + 1) * leaf_rows])
        for leaf in range(leaves)
    )
    state[0] = projected.astype(jnp.bfloat16)
    level_copy(0).start()

    loads[2].wait()
    loads[3].wait()
    rank_rows = lax.broadcasted_iota(jnp.int32, (rank, rank), 0)
    for level in range(levels):
        chosen = jnp.where(rank_rows == perm_ref[level : level + 1, :], 1.0, 0.0)
        partner_transfer[level] = dot(
            transfer_ref[0, level, 1], chosen.astype(jnp.bfloat16), (1, 1)
        ).astype(jnp.bfloat16)

    loads[4].wait()
    loads[5].wait()
    for leaf in range(leaves):
        own = coords_ref[leaf].astype(jnp.float32)
        points[leaf + leaves] = own
        for axis in range(2):
            targets[leaf, axis] = jnp.broadcast_to(own[axis : axis + 1, :], (piece, leaf_rows)).T
    total[...] = jnp.zeros_like(total)

    factor = 0.25 / math.sqrt(leaf_rows)

    def scale(target, offset):
        inside = (me * leaves + target + offset >= 0) & (me * leaves + target + offset < count * leaves)
        found = near_ref[target, 0] == offset
        for slot in range(1, NB):
            found = found | (near_ref[target, slot] == offset)
        return jnp.where(found & inside, jnp.float32(factor), jnp.float32(0.0))

    def tile(target, source, c):
        columns = pl.ds(pl.multiple_of(c * piece, piece), piece)
        x = points[source + leaves, 0:1, columns]
        y = points[source + leaves, 1:2, columns]
        dx = targets[target, 0] - x
        dy = targets[target, 1] - y
        value = lax.rsqrt(dx * dx + dy * dy + SOFTENING) * scale(target, source - target)
        return value.astype(jnp.bfloat16)

    def rows_of(source, c):
        leaf = source % leaves
        rows = pl.ds(pl.multiple_of(leaf * leaf_rows + c * piece, piece), piece)
        ref = rhs_ref if 0 <= source < leaves else (below_ref if source < 0 else above_ref)
        return ref[rows, :]

    def near(target, sources, c):
        tiles = jnp.concatenate([tile(target, source, c) for source in sources], axis=1)
        block = jnp.concatenate([rows_of(source, c) for source in sources], axis=0)
        total[target] += dot(tiles, block)

    def near_own(low, high):
        @pl.loop(low, high)
        def _(c):
            for target in range(leaves):
                near(target, list(range(leaves)), c)

    done = 0
    for level in range(levels):
        own_part = dot(transfer_ref[0, level, 0], state[level])
        if done < PIECES:
            near_own(done, done + 1)
            done += 1
        level_copy(level).wait_recv()
        state[level + 1] = (
            own_part + dot(partner_transfer[level], partner_state[level])
        ).astype(jnp.bfloat16)
        if level + 1 < levels:
            level_copy(level + 1).start()
        if level == 0:

            @pl.when(relay_up)
            def _():
                for slot in range(slots):
                    to_relay(rows_down(0), relay_send.at[slot], slot, up).wait_recv()
                    onward_up(slot).start()

            @pl.when(relay_down)
            def _():
                for slot in range(slots):
                    to_relay(rows_down(0), relay_send.at[slot], slot, up).wait_recv()
                    onward_down(slot).start()

        if level + 1 == LW:
            send_halo(FIRST, FIRST + SECOND)
        if level + 1 == LW + 1:
            send_halo(FIRST + SECOND, leaves * PIECES)
    loads[6].wait()
    for leaf in range(leaves):
        total[leaf] += dot(expand_ref[leaf], state[levels], (0, 0))

    @pl.when(not_first)
    def _():
        points_up.wait_recv()

    @pl.when(not_last)
    def _():
        points_down.wait_recv()

    for leaf in range(leaves):
        points[leaf] = below_raw[leaf].astype(jnp.float32)
        points[leaf + 2 * leaves] = above_raw[leaf].astype(jnp.float32)

    for phase in range(leaves):
        low, high = -1 - phase, leaves + phase

        @pl.loop(0, PIECES)
        def _(c):
            at = phase * PIECES + c

            @pl.when(not_first)
            def _():
                copy_up(at).wait_recv()

            @pl.when(not_last)
            def _():
                copy_down(at).wait_recv()

            for target in range(leaves):
                sources = [s for s in (low, high) if abs(s - target) <= leaves]
                near(target, sources, c)

    out_ref[...] = total[...].astype(out_ref.dtype)

    for level in range(levels):
        level_copy(level).wait_send()

    @pl.when(relay_up)
    def _():
        for slot in range(slots):
            onward_up(slot).wait_send()

    @pl.when(relay_down)
    def _():
        for slot in range(slots):
            onward_down(slot).wait_send()

    @pl.when(not_last)
    def _():
        points_up.wait_send()

        @pl.loop(0, leaves * PIECES)
        def _(c):
            copy_up(c).wait_send()

    @pl.when(not_first)
    def _():
        points_down.wait_send()

        @pl.loop(0, leaves * PIECES)
        def _(c):
            copy_down(c).wait_send()


def on_device(sizes, rhs, coords, near_index, project_basis, expand_basis, transfer, level_perm):
    leaves, _, leaf_rows = coords.shape
    rows, columns = rhs.shape
    levels, rank = level_perm.shape
    pieces = leaves * PIECES
    slots = sizes[0] // 2 - 1
    dma = pltpu.SemaphoreType.DMA
    vmem = pl.BlockSpec(memory_space=pltpu.VMEM)
    hbm = pl.BlockSpec(memory_space=pltpu.HBM)
    operands = (
        near_index,
        rhs,
        coords,
        project_basis.swapaxes(1, 2),
        expand_basis.swapaxes(1, 2),
        transfer,
        level_perm,
    )
    out = pl.pallas_call(
        functools.partial(kernel, sizes),
        out_shape=pltpu.VMEM((leaves, leaf_rows, columns), jnp.bfloat16),
        in_specs=[hbm] * len(operands),
        out_specs=vmem,
        scratch_shapes=[pltpu.SMEM(near_index.shape, near_index.dtype)]
        + [pltpu.VMEM(operand.shape, operand.dtype) for operand in operands[1:]]
        + [
            dma((len(operands),)),
            pltpu.VMEM((rows, columns), jnp.bfloat16),
            pltpu.VMEM((rows, columns), jnp.bfloat16),
            pltpu.VMEM(coords.shape, coords.dtype),
            pltpu.VMEM(coords.shape, coords.dtype),
            pltpu.VMEM((3 * leaves, 2, leaf_rows), jnp.float32),
            pltpu.VMEM((leaves, 2, leaf_rows, leaf_rows // PIECES), jnp.float32),
            pltpu.VMEM((leaves, leaf_rows, columns), jnp.float32),
            pltpu.VMEM((levels + 1, rank, columns), jnp.bfloat16),
            pltpu.VMEM((levels, rank, columns), jnp.bfloat16),
            pltpu.VMEM((levels, rank, rank), jnp.bfloat16),
            dma((pieces,)),
            dma((pieces,)),
            dma((pieces,)),
            dma((pieces,)),
            dma((2,)),
            dma((2,)),
            dma((levels,)),
            dma((levels,)),
            pltpu.VMEM((slots, leaf_rows // PIECES, columns), jnp.bfloat16),
            dma((slots,)),
            dma((slots,)),
        ],
        compiler_params=pltpu.CompilerParams(
            collective_id=0, has_side_effects=True, vmem_limit_bytes=VMEM_GRANT
        ),
        name="operator",
    )(*operands)
    return out.reshape(rows, columns)


def solution(mesh):
    sizes = (mesh.shape["wide"], mesh.shape["pair"])
    return jax.shard_map(
        functools.partial(on_device, sizes),
        mesh=mesh,
        in_specs=(
            P(("wide", "pair"), None),
            P(("wide", "pair"), None, None),
            P(("wide", "pair"), None),
            P(("wide", "pair"), None, None),
            P(("wide", "pair"), None, None),
            P(("wide", "pair"), None, None, None, None),
            P(),
        ),
        out_specs=P(("wide", "pair"), None),
        check_vma=False,
    )
```
